512 devices in a mesh: date: 64 (over z, y), prod: 8 (over x, core).
Axes of the slice: x: 4, y: 4, z: 16, core: 2. Of those that a mesh axis runs over, the one named last changes fastest.
Arguments:
- daily_sales: float32 [256, 2048, 128], P('prod', 'date'), may hold values from -2.5 to 2.5
- week_id: int32 [2048], P('date'), may hold values from 0 to 409, never falling along the last dimension, each value on 1 to 7 neighbouring positions
- month_id: int32 [2048], P('date'), may hold values from 0 to 85, never falling along the last dimension, each value on 1 to 31 neighbouring positions
- year_id: int32 [2048], P('date'), may hold values from 0 to 6, never falling along the last dimension, each value on 1 to 366 neighbouring positions
Outputs:
- running: float32 [256, 2048, 128], P('prod', 'date')
- week_total: float32 [256, 2048, 128], P('prod', 'date')
- month_total: float32 [256, 2048, 128], P('prod', 'date')
- year_total: float32 [256, 2048, 128], P('prod', 'date')
- store_rollup: float32 [4, 2048, 128], P(None, 'date')
The draws below stay inside these ranges and needn't reach their ends.
Inputs may be any that keep to these rules, and one draw needn't show every extreme that they name: `week_id`: starts at 0 and never falls along the dates; each week covers 1 to 7 consecutive dates and some cover exactly 7. `month_id`: starts at 0 and never falls along the dates; each month covers 1 to 31 consecutive dates and some cover exactly 31; months need not line up with weeks. `year_id`: starts at 0 and never falls along the dates; each year covers 1 to 366 consecutive dates and some cover exactly 366; years need not line up with weeks or months.
All inputs are finite; a program needn't handle non-finite values.
Results may differ from the reference program's by a relative error of at most 0.000094.
Values sent between devices are 32-bit elements.
A program may use at most 64 MiB of HBM per device.

```python
import math
import jax
import jax.numpy as jnp
import numpy as np

PRODUCTS = 256
STORES = 128
DATES = 2048


def shard_levels(stream_key, extent, split, low, high):
    loudness = 1.0
    for position, shards_of in split:
        steps = jax.random.uniform(jax.random.fold_in(jax.random.fold_in(stream_key, 6), position), (shards_of,), jnp.float32, low / len(split), high / len(split))
        loudness = loudness * jnp.repeat(jnp.exp(steps), extent[position] // shards_of).reshape((-1,) + (1,) * (len(extent) - 1 - position))
    return loudness


def split_up(number_of, total, reach, lean):
    portions = [(1 << 20) // math.isqrt(rank ** lean) + 1 for rank in range(2, number_of + 1)]
    rest, holding = total - reach - (number_of - 1), [1] * (number_of - 1)
    while rest > 0:
        movable = [i for i in range(number_of - 1) if holding[i] < reach]
        mass, remaining = sum([portions[i] for i in movable]), rest
        for i in movable:
            extra = min(reach - holding[i], max(1, remaining * portions[i] // mass), rest)
            holding[i] = holding[i] + extra
            rest = rest - extra
    return np.array([reach] + holding)


def uneven_parts(stream_key, amount, total, limit, slope):
    if amount == 2:
        one = jax.random.randint(stream_key, (), max(1, total - limit), min(limit, total - 1) + 1)
        return jnp.stack([one, total - one])
    tallies = jnp.asarray(split_up(amount, total, limit, slope), jnp.int32)
    pairs = (amount - 1) // 2
    giver, sink = tallies[1:1 + 2 * pairs:2], tallies[2:2 + 2 * pairs:2]
    room = jnp.minimum(giver - 1, limit - sink)
    passed = jax.random.randint(jax.random.fold_in(stream_key, 1), (pairs,), 0, 1 << 20) % (room + 1)
    tallies = tallies.at[1:1 + 2 * pairs:2].set(giver - passed).at[2:2 + 2 * pairs:2].set(sink + passed)
    return tallies[jax.random.permutation(jax.random.fold_in(stream_key, 2), amount)]


def normal_values(own_key, shape, deviation, limit, pieces=(), kind=jnp.bfloat16):
    factor_of = shard_levels(own_key, shape, pieces, -0.22, 0.18) if pieces else 1.0
    result = jax.random.normal(own_key, shape, jnp.float32) * deviation * factor_of
    return jnp.minimum(jnp.maximum(result, -limit), limit).astype(kind)


def setup_inputs(seed: int = 0) -> dict:
    seeds = jax.random.split(jax.random.key(seed), 5)
    return {
        "daily_sales": normal_values(seeds[0], (PRODUCTS, DATES, STORES), 0.25, 2.5, ((0, 8), (1, 64)), jnp.float32),
        "week_id": jnp.searchsorted(jnp.cumsum(uneven_parts(seeds[1], DATES // 5 + 1, DATES, 7, 0)), jnp.arange(DATES), side="right").astype(jnp.int32),
        "month_id": jnp.searchsorted(jnp.cumsum(uneven_parts(seeds[2], DATES // 24 + 1, DATES, 31, 0)), jnp.arange(DATES), side="right").astype(jnp.int32),
        "year_id": jnp.searchsorted(jnp.cumsum(uneven_parts(seeds[3], DATES // 300 + 1, DATES, 366, 0)), jnp.arange(DATES), side="right").astype(jnp.int32),
    }


def segment_totals(daily_sales, level_ids):
    by_date = jnp.moveaxis(daily_sales, 1, 0)
    seg_sums = jax.ops.segment_sum(by_date, level_ids, num_segments=DATES)
    return jnp.moveaxis(seg_sums[level_ids], 0, 1)


def reference(daily_sales, week_id, month_id, year_id):
    running = jnp.cumsum(daily_sales, axis=1)
    week_total = segment_totals(daily_sales, week_id)
    month_total = segment_totals(daily_sales, month_id)
    year_total = segment_totals(daily_sales, year_id)
    store_rollup = jnp.stack([jnp.sum(running, axis=0), jnp.sum(week_total, axis=0), jnp.sum(month_total, axis=0), jnp.sum(year_total, axis=0)])
    return running, week_total, month_total, year_total, store_rollup
```

```python
import functools

import jax
import jax.numpy as jnp
from jax import lax
from jax.experimental import pallas as pl
from jax.experimental.pallas import tpu as pltpu
from jax.sharding import PartitionSpec as P

MESH = pl.DeviceIdType.MESH
F32 = jnp.float32
I32 = jnp.int32

NZ, NY, NX, NC = 16, 4, 4, 2
REACH = 4
OFFS = (-4, -3, -2, -1, 1, 2, 3, 4)
SLOT = {o: i for i, o in enumerate(OFFS)}
SPAN = 32
COLS = 32
L = 128

RUN, WIN, MIN, YIN, WBK, MBK, YBK = range(7)


def spread(ids):
    sub = lax.broadcasted_iota(I32, (8, L), 0)
    tiles = []
    for j in range(SPAN // 8):
        v = jnp.full((8, L), ids[8 * j], I32)
        for r in range(1, 8):
            v = jnp.where(sub == r, ids[8 * j + r], v)
        tiles.append(v)
    return jnp.concatenate(tiles, axis=0)


def row_of(scalar):
    return jnp.full((1, L), scalar, I32).astype(F32)


def gate(cond):
    return jnp.where(cond, 1.0, 0.0).astype(F32)


def same(a, b):
    return jnp.where(a == b, 1.0, 0.0).astype(F32)


def stack_rows(rows):
    sub = lax.broadcasted_iota(I32, (8, L), 0)
    out = jnp.zeros((8, L), F32)
    for r, row in enumerate(rows):
        if row is not None:
            out = jnp.where(sub == r, row, out)
    return out


def exchange(
    wk, mo, yr, x_hbm, carry, glob,
    xv, a_out, a_in, w_out, w_in, p_out, p_in, x_in,
    b_out, b_in, b2_out, b2_in, c1_out, c1_in, c2_out, c2_in,
    g_out, g_in, gb_out, gb_in, gb2_out, gb2_in,
    ld_sem, send_sem, a_sem, w_sem, p_sem, x_sem, b_sem, b2_sem, c1_sem, c2_sem,
    g_sem, gb_sem, gb2_sem,
):
    d = lax.axis_index("date")
    pr = lax.axis_index("prod")
    z, y = lax.div(d, NY), lax.rem(d, NY)
    xx, core = lax.div(pr, NC), lax.rem(pr, NC)

    loads = [
        pltpu.make_async_copy(x_hbm.at[pl.ds(8 * q, 8)], xv.at[pl.ds(8 * q, 8)], ld_sem.at[q])
        for q in range(4)
    ]
    for cp in loads:
        cp.start()

    def y_dev(j):
        return z * NY + lax.rem(y + j, NY)

    def z_pos(k):
        return lax.rem(z + k + NZ, NZ)

    def z_dev(k):
        return z_pos(k) * NY + y

    def x_dev(j):
        return lax.rem(xx + j, NX) * NC + core

    after = lax.rem(d + 1, NZ * NY)
    ahead = lax.rem(d + NZ * NY - 1, NZ * NY)
    mate = xx * NC + (1 - core)

    barrier = pltpu.get_barrier_semaphore()
    partners = [(z_dev(k), pr) for k in (4, -4, 3, -3, 2, -2, 1, -1)]
    partners += [(y_dev(j), pr) for j in (2, 1, 3)]
    partners += [(d, x_dev(j)) for j in (2, 1, 3)]
    partners += [(d, mate), (after, pr), (ahead, pr)]
    for dev in partners:
        pl.semaphore_signal(barrier, inc=1, device_id=dev, device_id_type=MESH)

    sends = []

    def send(src, dst, sem, dev):
        cp = pltpu.make_async_remote_copy(
            src_ref=src, dst_ref=dst, send_sem=send_sem.at[len(sends)], recv_sem=sem,
            device_id=dev, device_id_type=MESH,
        )
        cp.start()
        sends.append(cp)

    def landed(ref, sem):
        pltpu.make_async_remote_copy(
            src_ref=ref, dst_ref=ref, send_sem=send_sem.at[0], recv_sem=sem,
            device_id=(d, pr), device_id_type=MESH,
        ).wait_recv()

    wid, mid, yid = spread(wk), spread(mo), spread(yr)
    wf, wl = wk[0], wk[SPAN - 1]
    mf, ml = mo[0], mo[SPAN - 1]
    yf, yl = yr[0], yr[SPAN - 1]
    wt_m, wh_m = gate(wid == wl), gate(wid == wf)
    mt_m, mh_m = gate(mid == ml), gate(mid == mf)
    yt_m, yh_m = gate(yid == yl), gate(yid == yf)
    wf_r, wl_r, mf_r, ml_r, yf_r, yl_r = (row_of(v) for v in (wf, wl, mf, ml, yf, yl))
    y_ids = stack_rows([yf_r, yl_r])

    for q in range(4):
        loads[q].wait()
        v = xv[pl.ds(8 * q, 8)]
        a_out[q, 0:8] = jnp.sum(v, axis=1)
        a_out[q, 8:16] = jnp.sum(v * yt_m[None], axis=1)
        a_out[q, 16:24] = jnp.sum(v * yh_m[None], axis=1)
        a_out[q, 24:32] = y_ids
    p_out[...] = jnp.sum(xv[...], axis=0)

    pl.semaphore_wait(barrier, len(partners))

    for j in (2, 1, 3):
        q = lax.rem(y + j, NY)
        send(a_out.at[q], a_in.at[y], a_sem.at[y], (y_dev(j), pr))
    send(p_out, p_in, p_sem.at[0], (d, mate))
    a_in[y] = a_out[y]

    for q in range(4):
        v = xv[pl.ds(8 * q, 8)]
        w_out[0, pl.ds(8 * q, 8)] = jnp.sum(v * wt_m[None], axis=1)
        w_out[0, pl.ds(32 + 8 * q, 8)] = jnp.sum(v * mt_m[None], axis=1)
        w_out[1, pl.ds(8 * q, 8)] = jnp.sum(v * wh_m[None], axis=1)
        w_out[1, pl.ds(32 + 8 * q, 8)] = jnp.sum(v * mh_m[None], axis=1)
    w_out[0, 64:72] = stack_rows([wl_r, ml_r])
    w_out[1, 64:72] = stack_rows([wf_r, mf_r])
    send(w_out.at[0], w_in.at[0], w_sem.at[0], (after, pr))
    send(w_out.at[1], w_in.at[1], w_sem.at[1], (ahead, pr))

    landed(p_in, p_sem.at[0])
    x_in[xx] = p_out[...] + p_in[...]
    for j in (2, 1, 3):
        send(x_in.at[xx], x_in.at[xx], x_sem.at[xx], (d, x_dev(j)))

    for j in (1, 2, 3):
        i = lax.rem(y + j, NY)
        landed(a_in.at[i], a_sem.at[i])
    tot = [a_in[i, 0:8] for i in range(NY)]
    y_tail = [a_in[i, 8:16] for i in range(NY)]
    y_head = [a_in[i, 16:24] for i in range(NY)]
    first = [a_in[i, 24:25] for i in range(NY)]
    last = [a_in[i, 25:26] for i in range(NY)]
    t_all = (tot[0] + tot[1]) + (tot[2] + tot[3])
    b_out[0, 0:8] = t_all
    b_out[1, 0:8] = t_all
    b_out[0, 8:16] = sum(same(last[i], last[3]) * y_tail[i] for i in range(NY))
    b_out[1, 8:16] = sum(same(first[i], first[0]) * y_head[i] for i in range(NY))
    b_out[0, 16:24] = jnp.broadcast_to(last[3], (8, L))
    b_out[1, 16:24] = jnp.broadcast_to(first[0], (8, L))

    def spread_z(out, inn, sem, rows):
        for k in (4, -4, 3, -3, 2, -2, 1, -1):
            side, n = (0 if k > 0 else 1), rows[abs(k)]
            slot = SLOT[-k]
            send(
                out.at[side, pl.ds(0, n)], inn.at[slot, pl.ds(0, n)], sem.at[slot],
                (z_dev(k), pr),
            )

    def landed_z(inn, sem, rows):
        for o in (1, -1, 2, -2, 3, -3, 4, -4):
            landed(inn.at[SLOT[o], pl.ds(0, rows[abs(o)])], sem.at[SLOT[o]])

    b_rows = {1: 24, 2: 24, 3: 24, 4: 8}
    spread_z(b_out, b_in, b_sem, b_rows)

    for j in (1, 3, 2):
        i = lax.rem(xx + j, NX)
        landed(x_in.at[i], x_sem.at[i])
    day = (x_in[0] + x_in[1]) + (x_in[2] + x_in[3])
    glob[0:SPAN] = day

    def over(m):
        v = day if m is None else day * m
        return jnp.sum(v, axis=0, keepdims=True)

    g_out[0:8] = stack_rows([over(None), over(yt_m), over(yh_m), yf_r, yl_r])
    g_out[8:16] = stack_rows(
        [over(wt_m), over(mt_m), over(wh_m), over(mh_m), wf_r, wl_r, mf_r, ml_r]
    )
    g_in[y] = g_out[...]
    for j in (2, 1, 3):
        send(g_out, g_in.at[y], g_sem.at[y], (y_dev(j), pr))

    landed(w_in.at[0], w_sem.at[0])
    landed(w_in.at[1], w_sem.at[1])
    has_prev, has_next = gate(d > 0), gate(d < NZ * NY - 1)
    carry[WIN] = (has_prev * same(w_in[0, 64:65], wf_r)) * w_in[0, 0:32]
    carry[MIN] = (has_prev * same(w_in[0, 65:66], mf_r)) * w_in[0, 32:64]
    carry[WBK] = (has_next * same(w_in[1, 64:65], wl_r)) * w_in[1, 0:32]
    carry[MBK] = (has_next * same(w_in[1, 65:66], ml_r)) * w_in[1, 32:64]

    for j in (1, 3, 2):
        i = lax.rem(y + j, NY)
        landed(g_in.at[i], g_sem.at[i])
    g_tot = [g_in[i, 0:1] for i in range(NY)]
    g_first = [g_in[i, 3:4] for i in range(NY)]
    g_last = [g_in[i, 4:5] for i in range(NY)]
    g_tail = [g_in[i, 1:2] for i in range(NY)]
    g_head = [g_in[i, 2:3] for i in range(NY)]
    gb_out[0, 0:8] = stack_rows(
        [
            (g_tot[0] + g_tot[1]) + (g_tot[2] + g_tot[3]),
            sum(same(g_last[i], g_last[3]) * g_tail[i] for i in range(NY)),
            sum(same(g_first[i], g_first[0]) * g_head[i] for i in range(NY)),
            g_first[0],
            g_last[3],
        ]
    )
    gb_out[1, 0:8] = gb_out[0, 0:8]
    gb_out[0, 8:16] = g_in[3, 8:16]
    gb_out[1, 8:16] = g_in[0, 8:16]
    g_rows = {1: 16, 2: 8, 3: 8, 4: 8}
    spread_z(gb_out, gb_in, gb_sem, g_rows)

    def earlier(o, to):
        return gate(z_pos(o) < z_pos(to))

    landed_z(b_in, b_sem, b_rows)
    b_tot = {o: b_in[SLOT[o], 0:8] for o in OFFS}
    b2_out[0] = sum(earlier(o, REACH) * b_tot[o] for o in (-4, -3, -2, -1))
    b2_out[1] = sum(earlier(o, -REACH) * b_tot[o] for o in (1, 2, 3))
    send(b2_out.at[0], b2_in.at[0], b2_sem.at[0], (z_dev(REACH), pr))
    send(b2_out.at[1], b2_in.at[1], b2_sem.at[1], (z_dev(-REACH), pr))
    back = [gate(z + o >= 0) for o in (-1, -2, -3)]
    forth = [gate(z + o < NZ) for o in (1, 2, 3)]
    for i in range(NY):
        into = jnp.zeros((8, L), F32)
        out = jnp.zeros((8, L), F32)
        for n, o in enumerate((-1, -2, -3)):
            s = SLOT[o]
            into += (back[n] * same(b_in[s, 16:17], first[i])) * b_in[s, 8:16]
        for e in range(i):
            into += same(last[e], first[i]) * y_tail[e]
        for n, o in enumerate((1, 2, 3)):
            s = SLOT[o]
            out += (forth[n] * same(b_in[s, 16:17], last[i])) * b_in[s, 8:16]
        for e in range(i + 1, NY):
            out += same(first[e], last[i]) * y_head[e]
        c1_out[i, 0:8] = into
        c1_out[i, 8:16] = out
    for j in (2, 1, 3):
        i = lax.rem(y + j, NY)
        send(c1_out.at[i], c1_in.at[y], c1_sem.at[y], (y_dev(j), pr))
    c1_in[y] = c1_out[y]
    direct = sum(earlier(o, 0) * b_tot[o] for o in OFFS)

    landed_z(gb_in, gb_sem, g_rows)
    gb_tot = {o: gb_in[SLOT[o], 0:8] for o in OFFS}
    gb2_out[0] = sum(earlier(o, REACH) * gb_tot[o] for o in (-4, -3, -2, -1))
    gb2_out[1] = sum(earlier(o, -REACH) * gb_tot[o] for o in (1, 2, 3))
    send(gb2_out.at[0], gb2_in.at[0], gb2_sem.at[0], (z_dev(REACH), pr))
    send(gb2_out.at[1], gb2_in.at[1], gb2_sem.at[1], (z_dev(-REACH), pr))
    g_direct = sum(earlier(o, 0) * gb_tot[o] for o in OFFS)

    landed(b2_in.at[0], b2_sem.at[0])
    landed(b2_in.at[1], b2_sem.at[1])
    upto = direct + (b2_in[0] + b2_in[1])
    for i in range(NY):
        c2_out[i] = upto
        upto = upto + tot[i]
    for j in (2, 1, 3):
        i = lax.rem(y + j, NY)
        send(c2_out.at[i], c2_in.at[y], c2_sem.at[y], (y_dev(j), pr))
    c2_in[y] = c2_out[y]

    into = jnp.zeros((1, L), F32)
    out = jnp.zeros((1, L), F32)
    for n, o in enumerate((-1, -2, -3)):
        s = SLOT[o]
        into += (back[n] * same(gb_in[s, 4:5], yf_r)) * gb_in[s, 1:2]
    for n, o in enumerate((1, 2, 3)):
        s = SLOT[o]
        out += (forth[n] * same(gb_in[s, 3:4], yl_r)) * gb_in[s, 2:3]
    within = jnp.zeros((1, L), F32)
    for e in range(NY):
        before, later = gate(y > e), gate(y < e)
        into += (before * same(g_last[e], yf_r)) * g_tail[e]
        out += (later * same(g_first[e], yl_r)) * g_head[e]
        within += before * g_tot[e]
    prev = jnp.where(y > 0, g_in[lax.rem(y + 3, NY), 8:16], gb_in[SLOT[-1], 8:16])
    nxt = jnp.where(y < NY - 1, g_in[lax.rem(y + 1, NY), 8:16], gb_in[SLOT[1], 8:16])
    win = (has_prev * same(prev[5:6], wf_r)) * prev[0:1]
    min_ = (has_prev * same(prev[7:8], mf_r)) * prev[1:2]
    wbk = (has_next * same(nxt[4:5], wl_r)) * nxt[2:3]
    mbk = (has_next * same(nxt[6:7], ml_r)) * nxt[3:4]
    landed(gb2_in.at[0], gb2_sem.at[0])
    landed(gb2_in.at[1], gb2_sem.at[1])
    run = (g_direct + (gb2_in[0] + gb2_in[1]))[0:1] + within
    glob[SPAN:SPAN + 8] = stack_rows([run, win, min_, into, wbk, mbk, out])

    for j in (1, 3, 2):
        i = lax.rem(y + j, NY)
        landed(c1_in.at[i], c1_sem.at[i])
    for q in range(4):
        carry[YIN, pl.ds(8 * q, 8)] = c1_in[q, 0:8]
        carry[YBK, pl.ds(8 * q, 8)] = c1_in[q, 8:16]
    for j in (1, 3, 2):
        i = lax.rem(y + j, NY)
        landed(c2_in.at[i], c2_sem.at[i])
    for q in range(4):
        carry[RUN, pl.ds(8 * q, 8)] = c2_in[q]
    for cp in sends:
        cp.wait_send()


N_SENDS = 3 + 1 + 2 + 3 + 8 + 3 + 8 + 2 + 3 + 2 + 3


def finish(
    wk, mo, yr, x_ref, carry, glob, run_o, week_o, month_o, year_o, roll_o,
    ov, rv, o_sem, r_sem,
):
    outs = (run_o, week_o, month_o, year_o)
    lane = lax.broadcasted_iota(I32, (8, L), 1)
    upon = jnp.bitwise_and(lane, SPAN - 1)

    ids = [spread(r) for r in (wk, mo, yr)]
    rows = []
    date = lax.broadcasted_iota(I32, (SPAN, L), 0)
    rows.append(gate(jnp.broadcast_to(upon[0:1], (SPAN, L)) <= date))
    starts, ends = [], []
    for ref, down in zip((wk, mo, yr), ids):
        across = jnp.full((8, L), ref[0], I32)
        for u in range(1, SPAN):
            across = jnp.where(upon == u, ref[u], across)
        rows.append(gate(jnp.broadcast_to(across[0:1], (SPAN, L)) == down))
        starts.append(gate(down == ref[0]))
        ends.append(gate(down == ref[SPAN - 1]))
    mix = jnp.concatenate(rows, axis=0)[:, 0:3 * SPAN].astype(jnp.bfloat16)

    def sums(v):
        hi = v.astype(jnp.bfloat16)
        rest = v - hi.astype(F32)
        mid = rest.astype(jnp.bfloat16)
        low = (rest - mid.astype(F32)).astype(jnp.bfloat16)
        return jnp.dot(
            mix, jnp.concatenate([hi, mid, low], axis=0), preferred_element_type=F32
        )

    def put(res, row, store):
        store(0, res[0:SPAN] + row(RUN))
        for n in range(3):
            store(
                n + 1,
                res[SPAN * (n + 1):SPAN * (n + 2)]
                + starts[n] * row(WIN + n)
                + ends[n] * row(WBK + n),
            )

    def chunk(c):
        return [
            pltpu.make_async_copy(
                ov.at[k, pl.ds(8 * c, 8)], outs[k].at[pl.ds(8 * c, 8)], o_sem.at[k, c]
            )
            for k in range(4)
        ]

    for c in range(4):
        def body(i, _):
            p = 8 * c + 2 * i
            res = sums(jnp.concatenate([x_ref[p], x_ref[p + 1]], axis=1))
            for h in range(2):
                def store(k, v):
                    ov[k, p + h] = v

                put(
                    res[:, h * L:(h + 1) * L],
                    lambda k: carry[k, pl.ds(p + h, 1)],
                    store,
                )
            return 0

        lax.fori_loop(0, 4, body, 0, unroll=True)
        for cp in chunk(c):
            cp.start()

    res = sums(glob[0:SPAN])

    def store_roll(k, v):
        rv[k] = v

    put(res, lambda k: glob[SPAN + k:SPAN + k + 1], store_roll)
    roll = pltpu.make_async_copy(rv, roll_o, r_sem)
    roll.start()
    for c in range(4):
        for cp in chunk(c):
            cp.wait()
    roll.wait()


def local(daily_sales, week_id, month_id, year_id):
    smem = pl.BlockSpec(memory_space=pltpu.SMEM)
    vmem = pl.BlockSpec(memory_space=pltpu.VMEM)
    hbm = pl.BlockSpec(memory_space=pl.ANY)
    dma = pltpu.SemaphoreType.DMA
    carry, glob = pl.pallas_call(
        exchange,
        name="exchange",
        out_shape=(
            jax.ShapeDtypeStruct((7, COLS, L), F32),
            jax.ShapeDtypeStruct((SPAN + 8, L), F32),
        ),
        in_specs=[smem, smem, smem, hbm],
        out_specs=(vmem, vmem),
        scratch_shapes=[
            pltpu.VMEM((COLS, SPAN, L), F32),
            pltpu.VMEM((NY, 32, L), F32), pltpu.VMEM((NY, 32, L), F32),
            pltpu.VMEM((2, 72, L), F32), pltpu.VMEM((2, 72, L), F32),
            pltpu.VMEM((SPAN, L), F32), pltpu.VMEM((SPAN, L), F32),
            pltpu.VMEM((NX, SPAN, L), F32),
            pltpu.VMEM((2, 24, L), F32), pltpu.VMEM((8, 24, L), F32),
            pltpu.VMEM((2, 8, L), F32), pltpu.VMEM((2, 8, L), F32),
            pltpu.VMEM((NY, 16, L), F32), pltpu.VMEM((NY, 16, L), F32),
            pltpu.VMEM((NY, 8, L), F32), pltpu.VMEM((NY, 8, L), F32),
            pltpu.VMEM((16, L), F32), pltpu.VMEM((NY, 16, L), F32),
            pltpu.VMEM((2, 16, L), F32), pltpu.VMEM((8, 16, L), F32),
            pltpu.VMEM((2, 8, L), F32), pltpu.VMEM((2, 8, L), F32),
            dma((4,)), dma((N_SENDS,)), dma((NY,)), dma((2,)), dma((1,)), dma((NX,)),
            dma((8,)), dma((2,)), dma((NY,)), dma((NY,)),
            dma((NY,)), dma((8,)), dma((2,)),
        ],
        compiler_params=pltpu.CompilerParams(
            collective_id=0, has_side_effects=True, vmem_limit_bytes=8 * 1024 * 1024
        ),
    )(week_id, month_id, year_id, daily_sales)
    big = jax.ShapeDtypeStruct(daily_sales.shape, F32)
    return pl.pallas_call(
        finish,
        name="finish",
        out_shape=(big, big, big, big, jax.ShapeDtypeStruct((4, SPAN, L), F32)),
        in_specs=[smem, smem, smem, vmem, vmem, vmem],
        out_specs=(hbm,) * 5,
        scratch_shapes=[
            pltpu.VMEM((4, COLS, SPAN, L), F32), pltpu.VMEM((4, SPAN, L), F32),
            dma((4, 4)), dma,
        ],
        compiler_params=pltpu.CompilerParams(vmem_limit_bytes=16 * 1024 * 1024),
    )(week_id, month_id, year_id, daily_sales, carry, glob)


def solution(mesh):
    return jax.shard_map(
        local,
        mesh=mesh,
        in_specs=(P("prod", "date", None), P("date"), P("date"), P("date")),
        out_specs=(
            P("prod", "date", None),
            P("prod", "date", None),
            P("prod", "date", None),
            P("prod", "date", None),
            P(None, "date", None),
        ),
        check_vma=False,
    )
```
